32 devices in a mesh: row: 8 (over z, x), col: 4 (over y, core).
Axes of the slice: x: 2, y: 2, z: 4, core: 2. Of those that a mesh axis runs over, the one named last changes fastest.
Arguments:
- pair: bfloat16 [64, 64, 128], P('row', 'col'), may hold values from -6 to 6
- norm_in: float32 [128], replicated, may hold values from 0.1 to 1.9
- shift_in: float32 [128], replicated, may hold values from -3 to 3
- in_weight: bfloat16 [128, 640], replicated, may hold values from -0.5 to 0.5
- norm_out: float32 [128], replicated, may hold values from 0.1 to 1.9
- shift_out: float32 [128], replicated, may hold values from -3 to 3
- out_weight: bfloat16 [128, 128], replicated, may hold values from -0.5 to 0.5
Outputs:
- update: bfloat16 [64, 64, 128], P('row', 'col')
The draws below stay inside these ranges and needn't reach their ends.
All inputs are finite; a program needn't handle non-finite values.
Results may differ from the reference program's by a relative error of at most 0.0054.
Values may be sent and summed in bfloat16 or wider, within the bound.
A program may use at most 64 MiB of HBM per device.

```python
import jax
import jax.numpy as jnp
from jax import lax

C = 128
CH = 128
N = 64
ROWS = 8
N_ROW = 8


def block_levels(key, extent, split, smallest, high):
    loudness, own = 1.0, jax.random.fold_in(key, 6)
    for dim, blocks in split:
        heights = jnp.exp(jax.random.uniform(jax.random.fold_in(own, dim), (blocks,), jnp.float32, smallest / len(split), high / len(split)))
        loudness = loudness * jnp.repeat(heights, extent[dim] // blocks).reshape([-1 if axis == dim else 1 for axis in range(len(extent))])
    return loudness


def centred(key, extent, scale, bound, pieces=(), held_as=jnp.bfloat16):
    result = jax.random.normal(key, extent, jnp.float32) * scale
    if len(pieces) > 0:
        result = block_levels(key, extent, pieces, -0.22, 0.18) * result
    return jnp.clip(result, min=-bound, max=bound).astype(held_as)


def setup_inputs(seed: int = 0) -> dict:
    streams_of = jax.random.split(jax.random.key(seed), 8)
    return {
        "pair": centred(streams_of[0], (N, N, C), 1.0, 6.0, ((0, 8), (1, 4))),
        "norm_in": jnp.clip(1.0 + 0.18 * jax.random.normal(streams_of[1], (C,), jnp.float32), 0.1, 1.9),
        "shift_in": centred(streams_of[2], (C,), 0.5, 3.0, (), jnp.float32),
        "in_weight": centred(streams_of[3], (C, 4 * CH + C), C ** -0.5, 0.5),
        "norm_out": jnp.clip(1.0 + 0.18 * jax.random.normal(streams_of[4], (CH,), jnp.float32), 0.1, 1.9),
        "shift_out": centred(streams_of[5], (CH,), 0.5, 3.0, (), jnp.float32),
        "out_weight": centred(streams_of[6], (CH, C), CH ** -0.5, 0.5),
    }


EPSILON = 1e-05

def layer_norm(values, gain, shift):
    values = values.astype(jnp.float32)
    center = lax.optimization_barrier(jnp.mean(values, axis=-1, keepdims=True))
    spread = lax.optimization_barrier(jnp.mean(jnp.square(values - center), axis=-1, keepdims=True))
    return (values - center) * lax.rsqrt(spread + EPSILON) * gain + shift

def project_block(block, norm_in, shift_in, in_weight):
    normed = layer_norm(block, norm_in, shift_in).astype(jnp.bfloat16)
    projected = jnp.dot(normed.reshape(-1, C), in_weight, preferred_element_type=jnp.float32)
    left = (jax.nn.sigmoid(projected[:, :CH]) * projected[:, CH:2 * CH]).astype(jnp.bfloat16)
    right = (jax.nn.sigmoid(projected[:, 2 * CH:3 * CH]) * projected[:, 3 * CH:4 * CH]).astype(jnp.bfloat16)
    gate = jax.nn.sigmoid(projected[:, 4 * CH:])
    return (left, right, gate)

def reference(pair, norm_in, shift_in, in_weight, norm_out, shift_out, out_weight):
    blocks = pair.reshape(N_ROW, ROWS, N, C)
    left, right, gate = lax.map(lambda block: project_block(block, norm_in, shift_in, in_weight), blocks)
    left = left.reshape(N, N, CH).astype(jnp.float32)
    right = right.reshape(N, N, CH).astype(jnp.float32)
    gate = gate.reshape(N, N, C)
    mixed = jnp.einsum('kih,kjh->ijh', left, right)
    mixed_normed = layer_norm(mixed, norm_out, shift_out).astype(jnp.bfloat16)
    outward = jnp.dot(mixed_normed.reshape(-1, CH), out_weight, preferred_element_type=jnp.float32)
    return (gate * outward.reshape(N, N, C)).astype(jnp.bfloat16)
```

```python
import functools

import jax
import jax.numpy as jnp
from jax import lax
from jax.experimental import pallas as pl
from jax.experimental.pallas import tpu as pltpu
from jax.sharding import PartitionSpec as P

EPSILON = 1e-05
MESH = pl.DeviceIdType.MESH


def layer_norm(values, gain, shift):
    center = jnp.mean(values, axis=-1, keepdims=True)
    values = values - center
    spread = jnp.mean(jnp.square(values), axis=-1, keepdims=True)
    return values * lax.rsqrt(spread + EPSILON) * gain + shift


def fit(size, most):
    while size % most:
        most -= 1
    return most


def loop(count, body):
    if count == 1:
        body(0)
    else:
        pl.loop(0, count)(body)


def kernel(
    n_row, n_col, pair_ref, gain_in, shift_in, w_in, gain_out, shift_out, w_out, out_ref,
    left_own, left_all, right_all, gate_ref, mixed, left_send, left_recv, right_send, right_recv,
):
    rows, cols, channels = pair_ref.shape
    hidden = w_out.shape[0]
    groups = n_row // n_col
    r, c = lax.axis_index("row"), lax.axis_index("col")
    home = r // groups

    barrier = pltpu.get_barrier_semaphore()

    def greet(row, col):
        pl.semaphore_signal(barrier, inc=1, device_id=(row, col), device_id_type=MESH)

    @pl.loop(1, n_row)
    def _(d):
        greet(lax.rem(r + d, n_row), c)

    @pl.loop(0, n_row)
    def _(d):
        row = lax.rem(r + d, n_row)

        @pl.when(jnp.logical_or(row != r, home != c))
        def _():
            greet(row, home)

    step = fit(rows, max(1, 128 // cols))

    def project(t):
        at = pl.ds(t * step, step)
        block = pair_ref[at].reshape(step * cols, channels).astype(jnp.float32)
        normed = layer_norm(block, gain_in[...], shift_in[...]).astype(jnp.bfloat16)

        def part(index):
            return jnp.dot(
                normed, w_in[:, index * hidden : (index + 1) * hidden],
                preferred_element_type=jnp.float32,
            )

        left = (jax.nn.sigmoid(part(0)) * part(1)).astype(jnp.bfloat16).reshape(step, cols, hidden)
        for g in range(groups):
            left_own[g, at] = left[:, g * rows : (g + 1) * rows]
        right = (jax.nn.sigmoid(part(2)) * part(3)).astype(jnp.bfloat16)
        right_all[r, at] = right.reshape(step, cols, hidden)
        gate_ref[at] = jax.nn.sigmoid(part(4)).reshape(step, cols, channels)

    loop(rows // step, project)

    own = jnp.where(home == c, 1, 0)
    pl.semaphore_wait(barrier, n_row - 1 + groups * n_col - own)

    def right_copy(d):
        return pltpu.make_async_remote_copy(
            src_ref=right_all.at[r], dst_ref=right_all.at[r],
            send_sem=right_send.at[d], recv_sem=right_recv.at[r],
            device_id=(lax.rem(r + d, n_row), c), device_id_type=MESH,
        )

    def left_copy(g, d):
        return pltpu.make_async_remote_copy(
            src_ref=left_own.at[g], dst_ref=left_all.at[r],
            send_sem=left_send.at[g * n_col + d], recv_sem=left_recv.at[r],
            device_id=(c * groups + g, lax.rem(c + d, n_col)), device_id_type=MESH,
        )

    def each_left(act):
        for g in range(groups):
            @pl.loop(0, n_col)
            def _(d):
                @pl.when(jnp.logical_or(d != 0, r != c * groups + g))
                def _():
                    act(left_copy(g, d))

    each_left(lambda copy: copy.start())

    @pl.loop(1, n_row)
    def _(d):
        right_copy(d).start()

    for g in range(groups):
        @pl.when(r == c * groups + g)
        def _():
            left_all[r] = left_own[g]

    tile_k, tile_i, tile_j = fit(rows, 8), fit(rows, 8), fit(cols, 16)
    mixed[...] = jnp.zeros_like(mixed)

    def accumulate(s):
        def over_i(ti):
            def over_j(tj):
                here = (pl.ds(ti * tile_i, tile_i), pl.ds(tj * tile_j, tile_j))

                def over_k(tk):
                    ks = pl.ds(tk * tile_k, tile_k)
                    lefts = left_all[s, ks, here[0]].astype(jnp.float32)
                    rights = right_all[s, ks, here[1]].astype(jnp.float32)
                    total = mixed[here]
                    for k in range(tile_k):
                        total += lefts[k][:, None, :] * rights[k][None]
                    mixed[here] = total

                loop(rows // tile_k, over_k)

            loop(cols // tile_j, over_j)

        loop(rows // tile_i, over_i)

    @pl.loop(0, n_row)
    def _(d):
        s = lax.rem(r + n_row - d, n_row)

        @pl.when(d != 0)
        def _():
            pltpu.make_async_copy(right_all.at[s], right_all.at[s], right_recv.at[s]).wait()

        @pl.when(jnp.logical_or(d != 0, home != c))
        def _():
            pltpu.make_async_copy(left_all.at[s], left_all.at[s], left_recv.at[s]).wait()

        accumulate(s)

    def finish(t):
        at = pl.ds(t * step, step)
        normed = layer_norm(
            mixed[at].reshape(step * cols, hidden), gain_out[...], shift_out[...]
        ).astype(jnp.bfloat16)
        outward = jnp.dot(normed, w_out[...], preferred_element_type=jnp.float32)
        out_ref[at] = (gate_ref[at] * outward.reshape(step, cols, channels)).astype(jnp.bfloat16)

    loop(rows // step, finish)

    each_left(lambda copy: copy.wait_send())

    @pl.loop(1, n_row)
    def _(d):
        right_copy(d).wait_send()


def solution(mesh):
    n_row, n_col = mesh.shape["row"], mesh.shape["col"]

    def local(pair, norm_in, shift_in, in_weight, norm_out, shift_out, out_weight):
        rows, cols, channels = pair.shape
        hidden = out_weight.shape[0]
        groups = n_row // n_col
        vmem = pl.BlockSpec(memory_space=pltpu.VMEM)
        return pl.pallas_call(
            functools.partial(kernel, n_row, n_col),
            out_shape=jax.ShapeDtypeStruct((rows, cols, channels), jnp.bfloat16),
            in_specs=[vmem] * 7,
            out_specs=vmem,
            scratch_shapes=[
                pltpu.VMEM((groups, rows, rows, hidden), jnp.bfloat16),
                pltpu.VMEM((n_row, rows, rows, hidden), jnp.bfloat16),
                pltpu.VMEM((n_row, rows, cols, hidden), jnp.bfloat16),
                pltpu.VMEM((rows, cols, channels), jnp.float32),
                pltpu.VMEM((rows, cols, hidden), jnp.float32),
                pltpu.SemaphoreType.DMA((groups * n_col,)),
                pltpu.SemaphoreType.DMA((n_row,)),
                pltpu.SemaphoreType.DMA((n_row,)),
                pltpu.SemaphoreType.DMA((n_row,)),
            ],
            compiler_params=pltpu.CompilerParams(collective_id=0, has_side_effects=True),
        )(
            pair, norm_in.reshape(1, -1), shift_in.reshape(1, -1), in_weight,
            norm_out.reshape(1, -1), shift_out.reshape(1, -1), out_weight,
        )

    in_specs = (P("row", "col", None), P(), P(), P(), P(), P(), P())
    return jax.shard_map(
        local, mesh=mesh, in_specs=in_specs, out_specs=P("row", "col", None), check_vma=False
    )
```

```python
import functools

import jax
import jax.numpy as jnp
from jax import lax
from jax.experimental import pallas as pl
from jax.experimental.pallas import tpu as pltpu
from jax.sharding import PartitionSpec as P

EPSILON = 1e-05
MESH = pl.DeviceIdType.MESH


def layer_norm(values, gain, shift):
    center = jnp.mean(values, axis=-1, keepdims=True)
    values = values - center
    spread = jnp.mean(jnp.square(values), axis=-1, keepdims=True)
    return values * lax.rsqrt(spread + EPSILON) * gain + shift


def fit(size, most):
    while size % most:
        most -= 1
    return most


def loop(count, body):
    if count == 1:
        body(0)
    else:
        pl.loop(0, count)(body)


def kernel(
    n_row, n_col, *refs
):
    sources, out_ref, held, fetch_sem = refs[:7], refs[7], refs[8:15], refs[15]
    fetches = [
        pltpu.make_async_copy(source, target, fetch_sem.at[i])
        for i, (source, target) in enumerate(zip(sources, held))
    ]
    for fetch in fetches:
        fetch.start()
    body(n_row, n_col, fetches, *held, out_ref, *refs[16:])


def body(
    n_row, n_col, fetches, pair_ref, gain_in, shift_in, w_in, gain_out, shift_out, w_out, out_ref,
    left_own, left_all, right_all, gate_ref, mixed,
    left_send, left_pass, left_recv, right_send, right_pass, right_recv,
):
    rows, cols, channels = pair_ref.shape
    hidden = w_out.shape[0]
    groups = n_row // n_col
    lines, chips = n_row // 2, n_col // 2
    r, c = lax.axis_index("row"), lax.axis_index("col")
    home = r // groups
    u, x, core = r // 2, lax.rem(r, 2), lax.rem(c, 2)
    pair_row = r + 1 - 2 * x
    turn = jnp.where(2 * u < lines, 1, lines - 1)

    def line(d):
        return lax.rem(u + turn * d, lines)

    first = c // 2 == home // 2
    barrier = pltpu.get_barrier_semaphore()

    def greet(row, col):
        pl.semaphore_signal(barrier, inc=1, device_id=(row, col), device_id_type=MESH)

    greet(pair_row, c)
    for d in range(1, lines):
        greet(2 * line(d) + x, c)

    for p in range(2):
        @pl.when(jnp.logical_or(c // 2 != home // 2, p != core))
        def _():
            greet(r, home // 2 * 2 + p)

    @pl.when(first)
    def _():
        for d in range(lines):
            source = 2 * line(d) + core

            @pl.when(jnp.logical_or(source != r, home != c))
            def _():
                greet(source, home)

    step = fit(rows, max(1, 128 // cols))
    for fetch in fetches:
        fetch.wait()

    def project(t):
        at = pl.ds(t * step, step)
        block = pair_ref[at].reshape(step * cols, channels).astype(jnp.float32)
        normed = layer_norm(block, gain_in[...], shift_in[...]).astype(jnp.bfloat16)

        def part(index):
            return jnp.dot(
                normed, w_in[:, index * hidden : (index + 1) * hidden],
                preferred_element_type=jnp.float32,
            )

        left = (jax.nn.sigmoid(part(0)) * part(1)).astype(jnp.bfloat16).reshape(step, cols, hidden)
        for g in range(groups):
            left_own[g, at] = left[:, g * rows : (g + 1) * rows]
        right = (jax.nn.sigmoid(part(2)) * part(3)).astype(jnp.bfloat16)
        right_all[r, at] = right.reshape(step, cols, hidden)
        gate_ref[at] = jax.nn.sigmoid(part(4)).reshape(step, cols, channels)

    loop(rows // step, project)

    itself = jnp.logical_and(home == c, x == core)
    expected = lines + groups - jnp.where(itself, 1, 0) + jnp.where(first, n_col - 1, 0)
    pl.semaphore_wait(barrier, expected)

    def right_copy(d):
        return pltpu.make_async_remote_copy(
            src_ref=right_all.at[r], dst_ref=right_all.at[r],
            send_sem=right_send.at[d], recv_sem=right_recv.at[r],
            device_id=(2 * line(d) + x if d else pair_row, c), device_id_type=MESH,
        )

    def right_forward(d):
        source = 2 * line(d) + x
        return pltpu.make_async_remote_copy(
            src_ref=right_all.at[source], dst_ref=right_all.at[source],
            send_sem=right_pass.at[d], recv_sem=right_recv.at[source],
            device_id=(pair_row, c), device_id_type=MESH,
        )

    def each_right(act):
        for d in reversed(range(lines)):
            act(right_copy(d))

    def left_copy(g):
        return pltpu.make_async_remote_copy(
            src_ref=left_own.at[g], dst_ref=left_all.at[r],
            send_sem=left_send.at[g], recv_sem=left_recv.at[r],
            device_id=(c * groups + g, c // 2 * 2 + x), device_id_type=MESH,
        )

    def left_forward(d, to):
        source = 2 * line(d) + core
        return pltpu.make_async_remote_copy(
            src_ref=left_all.at[source], dst_ref=left_all.at[source],
            send_sem=left_pass.at[d * n_col + to], recv_sem=left_recv.at[source],
            device_id=(r, lax.rem(c + to, n_col)), device_id_type=MESH,
        )

    def each_left(act):
        for g in range(groups):
            @pl.when(jnp.logical_or(r != c * groups + g, x != core))
            def _():
                act(left_copy(g))

    def arrive(buffer, semaphore, source):
        pltpu.make_async_copy(buffer.at[source], buffer.at[source], semaphore.at[source]).wait()

    each_right(lambda copy: copy.start())
    each_left(lambda copy: copy.start())

    for g in range(groups):
        @pl.when(jnp.logical_and(r == c * groups + g, x == core))
        def _():
            left_all[r] = left_own[g]

    for d in range(lines):
        if d:
            arrive(right_all, right_recv, 2 * line(d) + x)
            right_forward(d).start()

        @pl.when(first)
        def _():
            source = 2 * line(d) + core

            @pl.when(jnp.logical_or(source != r, home != c))
            def _():
                arrive(left_all, left_recv, source)

            for to in range(1, n_col):
                left_forward(d, to).start()

    tile_k, tile_i, tile_j = fit(rows, 8), fit(rows, 8), fit(cols, 16)
    mixed[...] = jnp.zeros_like(mixed)

    def accumulate(s):
        def over_i(ti):
            def over_j(tj):
                here = (pl.ds(ti * tile_i, tile_i), pl.ds(tj * tile_j, tile_j))

                def over_k(tk):
                    ks = pl.ds(tk * tile_k, tile_k)
                    lefts = left_all[s, ks, here[0]].astype(jnp.float32)
                    rights = right_all[s, ks, here[1]].astype(jnp.float32)
                    total = mixed[here]
                    for k in range(tile_k):
                        total += lefts[k][:, None, :] * rights[k][None]
                    mixed[here] = total

                loop(rows // tile_k, over_k)

            loop(cols // tile_j, over_j)

        loop(rows // tile_i, over_i)

    for d in range(lines):
        arrive(left_all, left_recv, 2 * line(d) + 1 - core)

        @pl.when(jnp.logical_not(first))
        def _():
            arrive(left_all, left_recv, 2 * line(d) + core)

        arrive(right_all, right_recv, 2 * line(d) + 1 - x)

        @pl.loop(0, 2)
        def _(e):
            accumulate(2 * line(d) + e)

    def finish(t):
        at = pl.ds(t * step, step)
        normed = layer_norm(
            mixed[at].reshape(step * cols, hidden), gain_out[...], shift_out[...]
        ).astype(jnp.bfloat16)
        outward = jnp.dot(normed, w_out[...], preferred_element_type=jnp.float32)
        out_ref[at] = (gate_ref[at] * outward.reshape(step, cols, channels)).astype(jnp.bfloat16)

    loop(rows // step, finish)

    each_left(lambda copy: copy.wait_send())
    each_right(lambda copy: copy.wait_send())
    for d in range(lines):
        if d:
            right_forward(d).wait_send()

        @pl.when(first)
        def _():
            for to in range(1, n_col):
                left_forward(d, to).wait_send()


def solution(mesh):
    n_row, n_col = mesh.shape["row"], mesh.shape["col"]

    def local(pair, norm_in, shift_in, in_weight, norm_out, shift_out, out_weight):
        rows, cols, channels = pair.shape
        hidden = out_weight.shape[0]
        groups = n_row // n_col
        vmem = pl.BlockSpec(memory_space=pltpu.VMEM)
        return pl.pallas_call(
            functools.partial(kernel, n_row, n_col),
            out_shape=jax.ShapeDtypeStruct((rows, cols, channels), jnp.bfloat16),
            in_specs=[pl.BlockSpec(memory_space=pl.ANY)] * 7,
            out_specs=vmem,
            scratch_shapes=[
                pltpu.VMEM(pair.shape, pair.dtype),
                pltpu.VMEM((1, channels), jnp.float32),
                pltpu.VMEM((1, channels), jnp.float32),
                pltpu.VMEM(in_weight.shape, in_weight.dtype),
                pltpu.VMEM((1, hidden), jnp.float32),
                pltpu.VMEM((1, hidden), jnp.float32),
                pltpu.VMEM(out_weight.shape, out_weight.dtype),
                pltpu.SemaphoreType.DMA((7,)),
                pltpu.VMEM((groups, rows, rows, hidden), jnp.bfloat16),
                pltpu.VMEM((n_row, rows, rows, hidden), jnp.bfloat16),
                pltpu.VMEM((n_row, rows, cols, hidden), jnp.bfloat16),
                pltpu.VMEM((rows, cols, channels), jnp.float32),
                pltpu.VMEM((rows, cols, hidden), jnp.float32),
                pltpu.SemaphoreType.DMA((groups,)),
                pltpu.SemaphoreType.DMA((n_row // 2 * n_col,)),
                pltpu.SemaphoreType.DMA((n_row,)),
                pltpu.SemaphoreType.DMA((n_row // 2,)),
                pltpu.SemaphoreType.DMA((n_row // 2,)),
                pltpu.SemaphoreType.DMA((n_row,)),
            ],
            compiler_params=pltpu.CompilerParams(collective_id=0, has_side_effects=True),
        )(
            pair, norm_in.reshape(1, -1), shift_in.reshape(1, -1), in_weight,
            norm_out.reshape(1, -1), shift_out.reshape(1, -1), out_weight,
        )

    in_specs = (P("row", "col", None), P(), P(), P(), P(), P(), P())
    return jax.shard_map(
        local, mesh=mesh, in_specs=in_specs, out_specs=P("row", "col", None), check_vma=False
    )
```

```python
import functools

import jax
import jax.numpy as jnp
from jax import lax
from jax.experimental import pallas as pl
from jax.experimental.pallas import tpu as pltpu
from jax.sharding import PartitionSpec as P

EPSILON = 1e-05
MESH = pl.DeviceIdType.MESH


def layer_norm(values, gain, shift):
    center = jnp.mean(values, axis=-1, keepdims=True)
    values = values - center
    spread = jnp.mean(jnp.square(values), axis=-1, keepdims=True)
    return values * lax.rsqrt(spread + EPSILON) * gain + shift


def fit(size, most):
    while size % most:
        most -= 1
    return most


def loop(count, body):
    if count == 1:
        body(0)
    else:
        pl.loop(0, count)(body)


def kernel(
    n_row, n_col, *refs
):
    sources, out_ref, held, fetch_sem = refs[:7], refs[7], refs[8:15], refs[15]
    fetches = [
        pltpu.make_async_copy(source, target, fetch_sem.at[i])
        for i, (source, target) in enumerate(zip(sources, held))
    ]
    for fetch in fetches:
        fetch.start()
    body(n_row, n_col, fetches, *held, out_ref, *refs[16:])


def body(
    n_row, n_col, fetches, pair_ref, gain_in, shift_in, w_in, gain_out, shift_out, w_out, out_ref,
    left_own, left_all, right_all, gate_ref, mixed,
    left_send, left_pass, left_recv, right_send, right_pass, right_recv,
):
    rows, cols, channels = pair_ref.shape
    hidden = w_out.shape[0]
    groups = n_row // n_col
    lines, chips = n_row // 2, n_col // 2
    r, c = lax.axis_index("row"), lax.axis_index("col")
    home = r // groups
    u, x, core = r // 2, lax.rem(r, 2), lax.rem(c, 2)
    pair_row = r + 1 - 2 * x
    turn = jnp.where(2 * u < lines, 1, lines - 1)

    def line(d):
        return lax.rem(u + turn * d, lines)

    first = c // 2 == home // 2
    barrier = pltpu.get_barrier_semaphore()

    def greet(row, col):
        pl.semaphore_signal(barrier, inc=1, device_id=(row, col), device_id_type=MESH)

    greet(pair_row, c)
    for d in range(1, lines):
        greet(2 * line(d) + x, c)

    for p in range(2):
        @pl.when(jnp.logical_or(c // 2 != home // 2, p != core))
        def _():
            greet(r, home // 2 * 2 + p)

    @pl.when(first)
    def _():
        for d in range(lines):
            source = 2 * line(d) + core

            @pl.when(jnp.logical_or(source != r, home != c))
            def _():
                greet(source, home)

    step = fit(rows, max(1, 128 // cols))
    for fetch in fetches:
        fetch.wait()

    def project(t):
        at = pl.ds(t * step, step)
        block = pair_ref[at].reshape(step * cols, channels).astype(jnp.float32)
        normed = layer_norm(block, gain_in[...], shift_in[...]).astype(jnp.bfloat16)

        def part(index):
            return jnp.dot(
                normed, w_in[:, index * hidden : (index + 1) * hidden],
                preferred_element_type=jnp.float32,
            )

        left = (jax.nn.sigmoid(part(0)) * part(1)).astype(jnp.bfloat16).reshape(step, cols, hidden)
        for g in range(groups):
            left_own[g, at] = left[:, g * rows : (g + 1) * rows]
        right = (jax.nn.sigmoid(part(2)) * part(3)).astype(jnp.bfloat16)
        right_all[r, at] = right.reshape(step, cols, hidden)
        gate_ref[at] = jax.nn.sigmoid(part(4)).reshape(step, cols, channels)

    loop(rows // step, project)

    itself = jnp.logical_and(home == c, x == core)
    expected = lines + groups - jnp.where(itself, 1, 0) + jnp.where(first, n_col - 1, 0)
    pl.semaphore_wait(barrier, expected)

    def right_copy(d):
        return pltpu.make_async_remote_copy(
            src_ref=right_all.at[r], dst_ref=right_all.at[r],
            send_sem=right_send.at[d], recv_sem=right_recv.at[r],
            device_id=(2 * line(d) + x if d else pair_row, c), device_id_type=MESH,
        )

    def right_forward(d):
        source = 2 * line(d) + x
        return pltpu.make_async_remote_copy(
            src_ref=right_all.at[source], dst_ref=right_all.at[source],
            send_sem=right_pass.at[d], recv_sem=right_recv.at[source],
            device_id=(pair_row, c), device_id_type=MESH,
        )

    def each_right(act):
        for d in reversed(range(lines)):
            act(right_copy(d))

    def left_copy(g):
        return pltpu.make_async_remote_copy(
            src_ref=left_own.at[g], dst_ref=left_all.at[r],
            send_sem=left_send.at[g], recv_sem=left_recv.at[r],
            device_id=(c * groups + g, c // 2 * 2 + x), device_id_type=MESH,
        )

    def left_forward(d, to):
        source = 2 * line(d) + core
        return pltpu.make_async_remote_copy(
            src_ref=left_all.at[source], dst_ref=left_all.at[source],
            send_sem=left_pass.at[d * n_col + to], recv_sem=left_recv.at[source],
            device_id=(r, lax.rem(c + to, n_col)), device_id_type=MESH,
        )

    def each_left(act):
        for g in range(groups):
            @pl.when(jnp.logical_or(r != c * groups + g, x != core))
            def _():
                act(left_copy(g))

    def arrive(buffer, semaphore, source):
        pltpu.make_async_copy(buffer.at[source], buffer.at[source], semaphore.at[source]).wait()

    each_left(lambda copy: copy.start())
    each_right(lambda copy: copy.start())

    for g in range(groups):
        @pl.when(jnp.logical_and(r == c * groups + g, x == core))
        def _():
            left_all[r] = left_own[g]

    for d in range(lines):
        if d:
            arrive(right_all, right_recv, 2 * line(d) + x)
            right_forward(d).start()

        @pl.when(first)
        def _():
            source = 2 * line(d) + core

            @pl.when(jnp.logical_or(source != r, home != c))
            def _():
                arrive(left_all, left_recv, source)

            for to in range(1, n_col):
                left_forward(d, to).start()

    tile_k, tile_i, tile_j = fit(rows, 8), fit(rows, 8), fit(cols, 16)
    mixed[...] = jnp.zeros_like(mixed)

    def accumulate(s):
        def over_i(ti):
            def over_j(tj):
                here = (pl.ds(ti * tile_i, tile_i), pl.ds(tj * tile_j, tile_j))

                def over_k(tk):
                    ks = pl.ds(tk * tile_k, tile_k)
                    lefts = left_all[s, ks, here[0]].astype(jnp.float32)
                    rights = right_all[s, ks, here[1]].astype(jnp.float32)
                    total = mixed[here]
                    for k in range(tile_k):
                        total += lefts[k][:, None, :] * rights[k][None]
                    mixed[here] = total

                loop(rows // tile_k, over_k)

            loop(cols // tile_j, over_j)

        loop(rows // tile_i, over_i)

    for d in range(lines):
        arrive(left_all, left_recv, 2 * line(d) + 1 - core)

        @pl.when(jnp.logical_not(first))
        def _():
            arrive(left_all, left_recv, 2 * line(d) + core)

        arrive(right_all, right_recv, 2 * line(d) + 1 - x)

        @pl.loop(0, 2)
        def _(e):
            accumulate(2 * line(d) + e)

    def finish(t):
        at = pl.ds(t * step, step)
        normed = layer_norm(
            mixed[at].reshape(step * cols, hidden), gain_out[...], shift_out[...]
        ).astype(jnp.bfloat16)
        outward = jnp.dot(normed, w_out[...], preferred_element_type=jnp.float32)
        out_ref[at] = (gate_ref[at] * outward.reshape(step, cols, channels)).astype(jnp.bfloat16)

    loop(rows // step, finish)

    each_left(lambda copy: copy.wait_send())
    each_right(lambda copy: copy.wait_send())
    for d in range(lines):
        if d:
            right_forward(d).wait_send()

        @pl.when(first)
        def _():
            for to in range(1, n_col):
                left_forward(d, to).wait_send()


def solution(mesh):
    n_row, n_col = mesh.shape["row"], mesh.shape["col"]

    def local(pair, norm_in, shift_in, in_weight, norm_out, shift_out, out_weight):
        rows, cols, channels = pair.shape
        hidden = out_weight.shape[0]
        groups = n_row // n_col
        vmem = pl.BlockSpec(memory_space=pltpu.VMEM)
        return pl.pallas_call(
            functools.partial(kernel, n_row, n_col),
            out_shape=pltpu.VMEM((rows, cols, channels), jnp.bfloat16),
            in_specs=[pl.BlockSpec(memory_space=pl.ANY)] * 7,
            out_specs=vmem,
            scratch_shapes=[
                pltpu.VMEM(pair.shape, pair.dtype),
                pltpu.VMEM((1, channels), jnp.float32),
                pltpu.VMEM((1, channels), jnp.float32),
                pltpu.VMEM(in_weight.shape, in_weight.dtype),
                pltpu.VMEM((1, hidden), jnp.float32),
                pltpu.VMEM((1, hidden), jnp.float32),
                pltpu.VMEM(out_weight.shape, out_weight.dtype),
                pltpu.SemaphoreType.DMA((7,)),
                pltpu.VMEM((groups, rows, rows, hidden), jnp.bfloat16),
                pltpu.VMEM((n_row, rows, rows, hidden), jnp.bfloat16),
                pltpu.VMEM((n_row, rows, cols, hidden), jnp.bfloat16),
                pltpu.VMEM((rows, cols, channels), jnp.float32),
                pltpu.VMEM((rows, cols, hidden), jnp.float32),
                pltpu.SemaphoreType.DMA((groups,)),
                pltpu.SemaphoreType.DMA((n_row // 2 * n_col,)),
                pltpu.SemaphoreType.DMA((n_row,)),
                pltpu.SemaphoreType.DMA((n_row // 2,)),
                pltpu.SemaphoreType.DMA((n_row // 2,)),
                pltpu.SemaphoreType.DMA((n_row,)),
            ],
            compiler_params=pltpu.CompilerParams(collective_id=0, has_side_effects=True),
        )(
            pair, norm_in.reshape(1, -1), shift_in.reshape(1, -1), in_weight,
            norm_out.reshape(1, -1), shift_out.reshape(1, -1), out_weight,
        )

    in_specs = (P("row", "col", None), P(), P(), P(), P(), P(), P())
    return jax.shard_map(
        local, mesh=mesh, in_specs=in_specs, out_specs=P("row", "col", None), check_vma=False
    )
```

```python
import functools

import jax
import jax.numpy as jnp
from jax import lax
from jax.experimental import pallas as pl
from jax.experimental.pallas import tpu as pltpu
from jax.sharding import PartitionSpec as P

EPSILON = 1e-05
MESH = pl.DeviceIdType.MESH


def layer_norm(values, gain, shift):
    center = jnp.mean(values, axis=-1, keepdims=True)
    values = values - center
    spread = jnp.mean(jnp.square(values), axis=-1, keepdims=True)
    return values * lax.rsqrt(spread + EPSILON) * gain + shift


def fit(size, most):
    while size % most:
        most -= 1
    return most


def loop(count, body):
    if count == 1:
        body(0)
    else:
        pl.loop(0, count)(body)


def kernel(
    n_row, n_col, *refs
):
    sources, out_ref, held, fetch_sem = refs[:7], refs[7], refs[8:15], refs[15]
    fetches = [
        pltpu.make_async_copy(source, target, fetch_sem.at[i])
        for i, (source, target) in enumerate(zip(sources, held))
    ]
    for fetch in fetches:
        fetch.start()
    body(n_row, n_col, fetches, *held, out_ref, *refs[16:])


def body(
    n_row, n_col, fetches, pair_ref, gain_in, shift_in, w_in, gain_out, shift_out, w_out, out_ref,
    left_own, left_all, right_all, gate_ref, mixed,
    left_send, left_pass, left_recv, right_send, right_pass, right_recv,
):
    rows, cols, channels = pair_ref.shape
    hidden = w_out.shape[0]
    groups = n_row // n_col
    lines, chips = n_row // 2, n_col // 2
    r, c = lax.axis_index("row"), lax.axis_index("col")
    home = r // groups
    u, x, core = r // 2, lax.rem(r, 2), lax.rem(c, 2)
    pair_row = r + 1 - 2 * x
    turn = jnp.where(2 * u < lines, 1, lines - 1)

    def line(d):
        return lax.rem(u + turn * d, lines)

    first = c // 2 == home // 2
    barrier = pltpu.get_barrier_semaphore()

    def greet(row, col):
        pl.semaphore_signal(barrier, inc=1, device_id=(row, col), device_id_type=MESH)

    greet(pair_row, c)
    for d in range(1, lines):
        greet(2 * line(d) + x, c)

        @pl.when(jnp.abs(line(d) - u) > lines // 2)
        def _():
            greet(2 * line(d) + 1 - x, c)


    for p in range(2):
        @pl.when(jnp.logical_or(c // 2 != home // 2, p != core))
        def _():
            greet(r, home // 2 * 2 + p)

    @pl.when(first)
    def _():
        for d in range(lines):
            source = 2 * line(d) + core

            @pl.when(jnp.logical_or(source != r, home != c))
            def _():
                greet(source, home)

    step = fit(rows, max(1, 128 // cols))
    for fetch in fetches:
        fetch.wait()

    def project(t):
        at = pl.ds(t * step, step)
        block = pair_ref[at].reshape(step * cols, channels).astype(jnp.float32)
        normed = layer_norm(block, gain_in[...], shift_in[...]).astype(jnp.bfloat16)

        def part(index):
            return jnp.dot(
                normed, w_in[:, index * hidden : (index + 1) * hidden],
                preferred_element_type=jnp.float32,
            )

        left = (jax.nn.sigmoid(part(0)) * part(1)).astype(jnp.bfloat16).reshape(step, cols, hidden)
        for g in range(groups):
            left_own[g, at] = left[:, g * rows : (g + 1) * rows]
        right = (jax.nn.sigmoid(part(2)) * part(3)).astype(jnp.bfloat16)
        right_all[r, at] = right.reshape(step, cols, hidden)
        gate_ref[at] = jax.nn.sigmoid(part(4)).reshape(step, cols, channels)

    loop(rows // step, project)

    itself = jnp.logical_and(home == c, x == core)
    expected = lines + groups - jnp.where(itself, 1, 0) + jnp.where(first, n_col - 1, 0)
    for d in range(1, lines):
        expected += jnp.where(jnp.abs(line(d) - u) > lines // 2, 1, 0)
    pl.semaphore_wait(barrier, expected)

    def right_copy(d):
        return pltpu.make_async_remote_copy(
            src_ref=right_all.at[r], dst_ref=right_all.at[r],
            send_sem=right_send.at[d], recv_sem=right_recv.at[r],
            device_id=(2 * line(d) + x if d else pair_row, c), device_id_type=MESH,
        )

    def right_forward(d):
        source = 2 * line(d) + x
        return pltpu.make_async_remote_copy(
            src_ref=right_all.at[source], dst_ref=right_all.at[source],
            send_sem=right_pass.at[d], recv_sem=right_recv.at[source],
            device_id=(pair_row, c), device_id_type=MESH,
        )

    def far(d):
        return jnp.abs(line(d) - u) > lines // 2

    def right_cross(d):
        return pltpu.make_async_remote_copy(
            src_ref=right_all.at[r], dst_ref=right_all.at[r],
            send_sem=right_pass.at[d], recv_sem=right_recv.at[r],
            device_id=(2 * line(d) + 1 - x, c), device_id_type=MESH,
        )

    def each_cross(act):
        for d in range(1, lines):
            @pl.when(far(d))
            def _():
                act(right_cross(d))

    def each_right(act):
        for d in reversed(range(lines)):
            act(right_copy(d))

    def left_copy(g):
        return pltpu.make_async_remote_copy(
            src_ref=left_own.at[g], dst_ref=left_all.at[r],
            send_sem=left_send.at[g], recv_sem=left_recv.at[r],
            device_id=(c * groups + g, c // 2 * 2 + x), device_id_type=MESH,
        )

    def left_forward(d, to):
        source = 2 * line(d) + core
        return pltpu.make_async_remote_copy(
            src_ref=left_all.at[source], dst_ref=left_all.at[source],
            send_sem=left_pass.at[d * n_col + to], recv_sem=left_recv.at[source],
            device_id=(r, lax.rem(c + to, n_col)), device_id_type=MESH,
        )

    def each_left(act):
        for g in range(groups):
            @pl.when(jnp.logical_or(r != c * groups + g, x != core))
            def _():
                act(left_copy(g))

    def arrive(buffer, semaphore, source):
        pltpu.make_async_copy(buffer.at[source], buffer.at[source], semaphore.at[source]).wait()

    each_right(lambda copy: copy.start())
    each_left(lambda copy: copy.start())
    each_cross(lambda copy: copy.start())

    for g in range(groups):
        @pl.when(jnp.logical_and(r == c * groups + g, x == core))
        def _():
            left_all[r] = left_own[g]

    for d in range(lines):
        if d:
            arrive(right_all, right_recv, 2 * line(d) + x)

            @pl.when(jnp.logical_not(far(d)))
            def _():
                right_forward(d).start()


        @pl.when(first)
        def _():
            source = 2 * line(d) + core

            @pl.when(jnp.logical_or(source != r, home != c))
            def _():
                arrive(left_all, left_recv, source)

            for to in range(1, n_col):
                left_forward(d, to).start()

    tile_k, tile_i, tile_j = fit(rows, 8), fit(rows, 8), fit(cols, 16)
    mixed[...] = jnp.zeros_like(mixed)

    def accumulate(s):
        def over_i(ti):
            def over_j(tj):
                here = (pl.ds(ti * tile_i, tile_i), pl.ds(tj * tile_j, tile_j))

                def over_k(tk):
                    ks = pl.ds(tk * tile_k, tile_k)
                    lefts = left_all[s, ks, here[0]].astype(jnp.float32)
                    rights = right_all[s, ks, here[1]].astype(jnp.float32)
                    total = mixed[here]
                    for k in range(tile_k):
                        total += lefts[k][:, None, :] * rights[k][None]
                    mixed[here] = total

                loop(rows // tile_k, over_k)

            loop(cols // tile_j, over_j)

        loop(rows // tile_i, over_i)

    for d in range(lines):
        arrive(left_all, left_recv, 2 * line(d) + 1 - core)

        @pl.when(jnp.logical_not(first))
        def _():
            arrive(left_all, left_recv, 2 * line(d) + core)

        arrive(right_all, right_recv, 2 * line(d) + 1 - x)

        @pl.loop(0, 2)
        def _(e):
            accumulate(2 * line(d) + e)

    def finish(t):
        at = pl.ds(t * step, step)
        normed = layer_norm(
            mixed[at].reshape(step * cols, hidden), gain_out[...], shift_out[...]
        ).astype(jnp.bfloat16)
        outward = jnp.dot(normed, w_out[...], preferred_element_type=jnp.float32)
        out_ref[at] = (gate_ref[at] * outward.reshape(step, cols, channels)).astype(jnp.bfloat16)

    loop(rows // step, finish)

    each_left(lambda copy: copy.wait_send())
    each_right(lambda copy: copy.wait_send())
    each_cross(lambda copy: copy.wait_send())
    for d in range(lines):
        if d:

            @pl.when(jnp.logical_not(far(d)))
            def _():
                right_forward(d).wait_send()


        @pl.when(first)
        def _():
            for to in range(1, n_col):
                left_forward(d, to).wait_send()


def solution(mesh):
    n_row, n_col = mesh.shape["row"], mesh.shape["col"]

    def local(pair, norm_in, shift_in, in_weight, norm_out, shift_out, out_weight):
        rows, cols, channels = pair.shape
        hidden = out_weight.shape[0]
        groups = n_row // n_col
        vmem = pl.BlockSpec(memory_space=pltpu.VMEM)
        return pl.pallas_call(
            functools.partial(kernel, n_row, n_col),
            out_shape=pltpu.VMEM((rows, cols, channels), jnp.bfloat16),
            in_specs=[pl.BlockSpec(memory_space=pl.ANY)] * 7,
            out_specs=vmem,
            scratch_shapes=[
                pltpu.VMEM(pair.shape, pair.dtype),
                pltpu.VMEM((1, channels), jnp.float32),
                pltpu.VMEM((1, channels), jnp.float32),
                pltpu.VMEM(in_weight.shape, in_weight.dtype),
                pltpu.VMEM((1, hidden), jnp.float32),
                pltpu.VMEM((1, hidden), jnp.float32),
                pltpu.VMEM(out_weight.shape, out_weight.dtype),
                pltpu.SemaphoreType.DMA((7,)),
                pltpu.VMEM((groups, rows, rows, hidden), jnp.bfloat16),
                pltpu.VMEM((n_row, rows, rows, hidden), jnp.bfloat16),
                pltpu.VMEM((n_row, rows, cols, hidden), jnp.bfloat16),
                pltpu.VMEM((rows, cols, channels), jnp.float32),
                pltpu.VMEM((rows, cols, hidden), jnp.float32),
                pltpu.SemaphoreType.DMA((groups,)),
                pltpu.SemaphoreType.DMA((n_row // 2 * n_col,)),
                pltpu.SemaphoreType.DMA((n_row,)),
                pltpu.SemaphoreType.DMA((n_row // 2,)),
                pltpu.SemaphoreType.DMA((n_row // 2,)),
                pltpu.SemaphoreType.DMA((n_row,)),
            ],
            compiler_params=pltpu.CompilerParams(collective_id=0, has_side_effects=True),
        )(
            pair, norm_in.reshape(1, -1), shift_in.reshape(1, -1), in_weight,
            norm_out.reshape(1, -1), shift_out.reshape(1, -1), out_weight,
        )

    in_specs = (P("row", "col", None), P(), P(), P(), P(), P(), P())
    return jax.shard_map(
        local, mesh=mesh, in_specs=in_specs, out_specs=P("row", "col", None), check_vma=False
    )
```
